32 devices in a mesh: groups: 2 (over x), seq: 16 (over z, y, core).
Axes of the slice: x: 2, y: 2, z: 4, core: 2. Of those that a mesh axis runs over, the one named last changes fastest.
Arguments:
- queries: bfloat16 [4, 128, 8192], P(None, ('groups', 'seq')), parts along dimension 1, may hold values from -16 to 16
- new_keys: bfloat16 [4, 128, 1024], P(None, ('groups', 'seq')), parts along dimension 1, may hold values from -6 to 6
- new_values: bfloat16 [4, 128, 1024], P(None, ('groups', 'seq')), parts along dimension 1, may hold values from -6 to 6
- pool_keys: bfloat16 [2048, 16, 1024], P(('groups', 'seq')), parts along dimension 0, may hold values from -6 to 6
- pool_values: bfloat16 [2048, 16, 1024], P(('groups', 'seq')), parts along dimension 0, may hold values from -6 to 6
- page_table: int32 [128, 16], P(('groups', 'seq')), parts along dimension 0, may hold values from 0 to 63, as said below
- cached_len: int32 [128], P(('groups', 'seq')), parts along dimension 0, may hold values from 1 to 256
- turn_keys: bfloat16 [4, 32, 16, 1024], P(None, ('groups', 'seq')), parts along dimension 1, may hold values from -6 to 6
- turn_values: bfloat16 [4, 32, 16, 1024], P(None, ('groups', 'seq')), parts along dimension 1, may hold values from -6 to 6
- turn_lengths: int32 [32], P('groups'), parts along dimension 0, may hold values from 1 to 80, 768 in all
- turn_slot: int32 [32], P('groups'), parts along dimension 0, may hold values from 0 to 63, as said below
Outputs:
- attended: bfloat16 [4, 128, 8192], P(None, ('groups', 'seq')), parts along dimension 1
- landed_keys: bfloat16 [32, 80, 1024], P(('groups', 'seq')), parts along dimension 0
- landed_values: bfloat16 [32, 80, 1024], P(('groups', 'seq')), parts along dimension 0
The draws below stay inside these ranges and needn't reach their ends.
There are 2 independent parts, one for each index of `groups`. The reference program is written for one: setup_inputs(seed, part) draws one part's arguments, and reference() takes and returns one part's arrays. A program takes and returns all parts, laid end to end along the dimension named above; each array names one. Nothing has to cross between parts.
Inputs may be any that keep to these rules, and one draw needn't show every extreme that they name: `page_table`: the 4 rows of each device's slots together hold every number of 0 to 63 exactly once. `turn_lengths`: they sum to 768; the largest is exactly 80. `turn_slot`: each block of 4 slots holds the slot of exactly one turn.
All inputs are finite; a program needn't handle non-finite values.
Results may differ from the reference program's by a relative error of at most 0.0049.
Values may be sent and summed in bfloat16 or wider, within the bound.
A program may use at most 128 MiB of HBM per device.

```python
import math
import jax
import jax.numpy as jnp
import numpy as np
from jax import lax

QH = 64
KVH = 8
HD = 128
KV = 1024
PAGE = 16
STEPS = 4
SLOT_DEV = 4
CPAGES = 16
PG_DEV = 4
CHAIN = 16
TURNS = 16
SLOTS = 64
POOL_DEV = 64
POOL = 1024
PPAGES = 64
MOSTT = 80
TTOK = 768


key_level = 5.25


second_level = 5.21875


def draw_page_table(key, part):
    device_keys = jax.random.split(jax.random.fold_in(key, 11), CHAIN)

    def one_device(device_key):
        return jax.random.permutation(device_key, POOL_DEV)
    tables = jax.vmap(one_device)(device_keys)
    return tables.reshape(SLOTS, CPAGES).astype(jnp.int32)


def draw_turn_slot(key, part):
    owner_key, offset_key = jax.random.split(jax.random.fold_in(key, 23))
    owner_ids = jax.random.permutation(owner_key, CHAIN)[:TURNS]
    offsets = jax.random.randint(offset_key, (TURNS,), 0, SLOT_DEV)
    return (owner_ids * SLOT_DEV + offsets).astype(jnp.int32)


def drawn_parts(key):
    group_key, sign_key, level_key = jax.random.split(jax.random.fold_in(key, 77), 3)
    chosen = jax.random.randint(group_key, (SLOTS,), 0, KVH)
    signs = (2 * jax.random.randint(sign_key, (KVH, HD), 0, 2) - 1).astype(jnp.float32)
    levels = jax.random.uniform(level_key, (STEPS, SLOTS, QH // KVH), jnp.float32, 180.0, 320.0)
    return (chosen, signs, levels)


def base_draw(key, shape):
    return jax.random.truncated_normal(key, -6.0, 6.0, shape, jnp.float32)


def draw_queries(key, part):
    chosen, signs, levels = drawn_parts(key)
    group_share = QH // KVH
    base = base_draw(jax.random.fold_in(key, 5), (STEPS, SLOTS, KVH, group_share, HD))
    strength = levels / (key_level * math.sqrt(HD))
    planted = strength[:, :, None, :, None] * signs[None, None, :, None, :]
    in_group = jnp.arange(KVH)[None, :] == chosen[:, None]
    later = jnp.arange(STEPS) >= 1
    using = later[:, None, None] & in_group[None, :, :]
    mixed = jnp.where(using[..., None, None], planted, base)
    return mixed.reshape(STEPS, SLOTS, QH * HD).astype(jnp.bfloat16)


def draw_new_keys(key, part):
    chosen, signs, levels = drawn_parts(key)
    base = base_draw(jax.random.fold_in(key, 6), (STEPS, SLOTS, KVH, HD))
    step_level = jnp.where(jnp.arange(STEPS) == 0, key_level, second_level).astype(jnp.float32)
    planted = step_level[:, None, None, None] * signs[None, None, :, :]
    in_group = jnp.arange(KVH)[None, :] == chosen[:, None]
    early = jnp.arange(STEPS) <= 1
    using = early[:, None, None] & in_group[None, :, :]
    mixed = jnp.where(using[..., None], planted, base)
    return mixed.reshape(STEPS, SLOTS, KV).astype(jnp.bfloat16)


def plant(entries, own_key, least, high):
    place = [jax.random.randint(jax.random.fold_in(own_key, axis), (), 0, length) for axis, length in enumerate(entries.shape)]
    main_axis = entries.shape.index(max(entries.shape))
    next_to = place[:main_axis] + [(place[main_axis] + 1) % entries.shape[main_axis]] + place[main_axis + 1:]
    return entries.at[tuple(place)].set(least).at[tuple(next_to)].set(high)


def block_scale(own_key, extent, cuts, low, top_value):
    factor_of = 1.0
    for dim, parts in cuts:
        heights = jax.random.uniform(jax.random.fold_in(jax.random.fold_in(own_key, 6), dim), (parts,), jnp.float32, low / len(cuts), top_value / len(cuts))
        factor_of = factor_of * jnp.repeat(jnp.exp(heights), extent[dim] // parts).reshape((-1,) + (1,) * (len(extent) - 1 - dim))
    return factor_of


def split_up(number_of, total, most, skew):
    portions = [(1 << 20) // math.isqrt(grade ** skew) + 1 for grade in range(2, number_of + 1)]
    spare, counts = total - most - (number_of - 1), [1] * (number_of - 1)
    while spare > 0:
        movable = [i for i in range(number_of - 1) if counts[i] < most]
        pool, left = sum([portions[i] for i in movable]), spare
        for i in movable:
            addition = min(most - counts[i], max(1, left * portions[i] // pool), spare)
            counts[i] = counts[i] + addition
            spare = spare - addition
    return np.array([most] + counts)


def uneven(rng, count, total, limit, lean):
    if count == 2:
        one = jax.random.randint(rng, (), max(1, total - limit), min(limit, total - 1) + 1)
        return jnp.stack([one, total - one])
    sizes = jnp.asarray(split_up(count, total, limit, lean), jnp.int32)
    twos = (count - 1) // 2
    donor, receiver = sizes[1:1 + 2 * twos:2], sizes[2:2 + 2 * twos:2]
    slack = jnp.minimum(donor - 1, limit - receiver)
    passed = jax.random.randint(jax.random.fold_in(rng, 1), (twos,), 0, 1 << 20) % (slack + 1)
    sizes = sizes.at[1:1 + 2 * twos:2].set(donor - passed).at[2:2 + 2 * twos:2].set(receiver + passed)
    return sizes[jax.random.permutation(jax.random.fold_in(rng, 2), count)]


def normal_values(stream_key, extent, width, reach, pieces=(), held_as=jnp.bfloat16):
    drawn = jax.random.normal(stream_key, extent, jnp.float32) * width
    if len(pieces) > 0:
        drawn = block_scale(stream_key, extent, pieces, -0.22, 0.18) * drawn
    return jnp.clip(drawn, min=-reach, max=reach).astype(held_as)


def setup_inputs(seed: int = 0, part: int = 0) -> dict:
    streams_of = jax.random.split(jax.random.key(seed), 12)
    part_keys = jax.random.split(jax.random.fold_in(streams_of[11], part), 12)
    queries = draw_queries(jax.random.fold_in(jax.random.fold_in(streams_of[11], part), 71), part)
    new_keys = draw_new_keys(jax.random.fold_in(jax.random.fold_in(streams_of[11], part), 71), part)
    new_values = normal_values(part_keys[2], (STEPS, SLOTS, KV), 1.0, 6.0, ((1, 16),))
    pool_keys = normal_values(part_keys[3], (POOL, PAGE, KV), 1.0, 6.0, ((0, 16),))
    pool_values = normal_values(part_keys[4], (POOL, PAGE, KV), 1.0, 6.0, ((0, 16),))
    page_table = draw_page_table(jax.random.fold_in(jax.random.fold_in(streams_of[11], part), 71), part)
    cached_len = plant(jax.random.randint(part_keys[6], (SLOTS,), 1, CPAGES * PAGE + 1), jax.random.fold_in(part_keys[6], 1), 1, CPAGES * PAGE).astype(jnp.int32)
    turn_keys = normal_values(part_keys[7], (PG_DEV, CHAIN, PAGE, KV), 1.0, 6.0, ((1, 16),))
    turn_values = normal_values(part_keys[8], (PG_DEV, CHAIN, PAGE, KV), 1.0, 6.0, ((1, 16),))
    turn_lengths = uneven(part_keys[9], TURNS, TTOK, MOSTT, 2).astype(jnp.int32)
    turn_slot = draw_turn_slot(jax.random.fold_in(jax.random.fold_in(streams_of[11], part), 71), part)
    return {"queries": queries, "new_keys": new_keys, "new_values": new_values, "pool_keys": pool_keys, "pool_values": pool_values, "page_table": page_table, "cached_len": cached_len, "turn_keys": turn_keys, "turn_values": turn_values, "turn_lengths": turn_lengths, "turn_slot": turn_slot}


def reference(queries, new_keys, new_values, pool_keys, pool_values, page_table, cached_len, turn_keys, turn_values, turn_lengths, turn_slot):
    page_counts = (turn_lengths + PAGE - 1) // PAGE
    page_starts = jnp.cumsum(page_counts) - page_counts
    owner_ids = turn_slot // SLOT_DEV
    padding = jnp.zeros((MOSTT, KV), jnp.bfloat16)
    packed_keys = jnp.concatenate([turn_keys.reshape(PPAGES * PAGE, KV), padding], axis=0)
    packed_values = jnp.concatenate([turn_values.reshape(PPAGES * PAGE, KV), padding], axis=0)
    landed_keys = jnp.zeros((CHAIN, MOSTT, KV), jnp.bfloat16)
    landed_values = jnp.zeros((CHAIN, MOSTT, KV), jnp.bfloat16)
    positions = jnp.arange(MOSTT, dtype=jnp.int32)
    for turn_index in range(TURNS):
        first_token = (page_starts[turn_index] * PAGE).astype(jnp.int32)
        keeping = (positions < turn_lengths[turn_index])[:, None]
        piece_keys = lax.dynamic_slice_in_dim(packed_keys, first_token, MOSTT, 0)
        piece_values = lax.dynamic_slice_in_dim(packed_values, first_token, MOSTT, 0)
        landed_keys = landed_keys.at[owner_ids[turn_index]].set(jnp.where(keeping, piece_keys, jnp.zeros_like(piece_keys)))
        landed_values = landed_values.at[owner_ids[turn_index]].set(jnp.where(keeping, piece_values, jnp.zeros_like(piece_values)))
    slot_ids = jnp.arange(SLOTS, dtype=jnp.int32)
    matches = turn_slot[None, :] == slot_ids[:, None]
    fresh_lengths = lax.optimization_barrier(jnp.sum(jnp.where(matches, turn_lengths[None, :], 0), axis=1)).astype(jnp.int32)
    score_scale = 1.0 / math.sqrt(HD)
    group_share = QH // KVH
    token_span = CPAGES * PAGE
    causal_mask = jnp.arange(STEPS)[None, :] <= jnp.arange(STEPS)[:, None]

    def attend_slot(inputs):
        query_rows, key_rows, value_rows, table_row, resident_len, fresh_len, slot_id = inputs
        owner_id = slot_id // SLOT_DEV
        pool_rows = owner_id * POOL_DEV + table_row
        resident_keys = pool_keys[pool_rows].reshape(token_span, KV)
        resident_values = pool_values[pool_rows].reshape(token_span, KV)
        fresh_keys = lax.dynamic_index_in_dim(landed_keys, owner_id, 0, keepdims=False)
        fresh_values = lax.dynamic_index_in_dim(landed_values, owner_id, 0, keepdims=False)
        all_keys = jnp.concatenate([resident_keys, fresh_keys, key_rows], axis=0).astype(jnp.float32).reshape(-1, KVH, HD)
        all_values = jnp.concatenate([resident_values, fresh_values, value_rows], axis=0).astype(jnp.float32).reshape(-1, KVH, HD)
        valid_resident = jnp.broadcast_to((jnp.arange(token_span) < resident_len)[None, :], (STEPS, token_span))
        valid_fresh = jnp.broadcast_to((jnp.arange(MOSTT) < fresh_len)[None, :], (STEPS, MOSTT))
        valid_all = jnp.concatenate([valid_resident, valid_fresh, causal_mask], axis=1)
        query_heads = query_rows.astype(jnp.float32).reshape(STEPS, KVH, group_share, HD)
        scores = jnp.einsum('sgeh,cgh->sgec', query_heads, all_keys) * score_scale
        scores = jnp.where(valid_all[:, None, None, :], scores, -jnp.inf)
        largest = lax.optimization_barrier(jnp.max(scores, axis=-1, keepdims=True))
        weights = jnp.exp(scores - largest)
        weights = weights / lax.optimization_barrier(jnp.sum(weights, axis=-1, keepdims=True))
        mixed = jnp.einsum('sgec,cgh->sgeh', weights, all_values)
        return mixed.reshape(STEPS, QH * HD).astype(jnp.bfloat16)
    per_slot = lax.map(attend_slot, (jnp.swapaxes(queries, 0, 1), jnp.swapaxes(new_keys, 0, 1), jnp.swapaxes(new_values, 0, 1), page_table, cached_len, fresh_lengths, slot_ids))
    attended = jnp.swapaxes(per_slot, 0, 1)
    return (attended, landed_keys, landed_values)
```

```python
import functools
import math

import jax
import jax.numpy as jnp
from jax import lax
from jax.experimental import pallas as pl
from jax.experimental.pallas import tpu as pltpu
from jax.sharding import PartitionSpec as P

QH = 64
KVH = 8
HD = 128
MOSTT = 80
SUB = 8
LANES = 128
NEG = -1e30
F32 = jnp.float32
BF16 = jnp.bfloat16


def kernel(
    n,
    table_ref,
    cached_ref,
    lengths_ref,
    slots_ref,
    q_hbm,
    nk_hbm,
    nv_hbm,
    pk_hbm,
    pv_hbm,
    tk_hbm,
    tv_hbm,
    out_ref,
    lk_ref,
    lv_ref,
    q_v,
    n_v,
    pk_v,
    pv_v,
    t_v,
    first_k,
    first_v,
    second,
    landing_k,
    landing_v,
    fresh,
    qf,
    of,
    acc,
    mx,
    sm,
    start_s,
    pick_s,
    load_sem,
    own_sem,
    send1,
    recv1,
    send2,
    recv2,
):
    me = lax.axis_index("seq")
    steps, slots_here, _ = q_hbm.shape
    group_pages, page_rows, kv_width = tk_hbm.shape
    pages_here = pk_hbm.shape[0]
    turns = lengths_ref.shape[0]
    cache_pages = table_ref.shape[1]
    lane_tiles = kv_width // LANES
    spread = (page_rows // SUB) * lane_tiles
    most_pages = -(-MOSTT // page_rows)
    fresh_span = most_pages * page_rows
    blocks = n // spread
    share = QH // KVH
    rows_sr = steps * slots_here
    my_block = me // spread
    first = (first_k, first_v)
    landing = (landing_k, landing_v)

    def load(index, src, dst):
        return pltpu.make_async_copy(src, dst, load_sem.at[index])

    loads = [
        load(0, tk_hbm, t_v.at[0]),
        load(1, tv_hbm, t_v.at[1]),
        load(2, q_hbm, q_v),
        load(3, pk_hbm, pk_v),
        load(4, pv_hbm, pv_v),
        load(5, nk_hbm, n_v.at[0]),
        load(6, nv_hbm, n_v.at[1]),
    ]
    for copy in loads:
        copy.start()

    barrier = pltpu.get_barrier_semaphore()

    @pl.loop(1, n)
    def _(k):
        pl.semaphore_signal(barrier, inc=1, device_id={"seq": lax.rem(me + k, n)})

    running = jnp.int32(0)
    my_length = jnp.int32(0)
    my_slot = jnp.int32(0)
    for t in range(turns):
        start_s[t] = running
        length = lengths_ref[t]
        slot = slots_ref[t]
        mine = lax.div(slot, slots_here) == me
        my_length = jnp.where(mine, length, my_length)
        my_slot = jnp.where(mine, lax.rem(slot, slots_here), my_slot)
        running = running + lax.div(length + (page_rows - 1), page_rows)

    @pl.loop(0, n)
    def _(d):
        begin = jnp.int32(0)
        for t in range(turns):
            begin = jnp.where(lax.div(slots_ref[t], slots_here) == d, start_s[t], begin)
        for j in range(most_pages):
            page = jnp.minimum(begin + j, group_pages * n - 1)
            row = lax.rem(lax.rem(page, n), spread) * group_pages + lax.div(page, n)
            pick_s[d * most_pages + j] = row

    def tile(h):
        t = lax.rem(h, spread)
        top = pl.multiple_of(lax.div(t, lane_tiles) * SUB, SUB)
        left = pl.multiple_of(lax.rem(t, lane_tiles) * LANES, LANES)
        return pl.ds(top, SUB), pl.ds(left, LANES)

    def slot_of(src):
        return pl.ds(lax.rem(src, spread) * group_pages, group_pages)

    def hand1(a, k):
        h = my_block * spread + lax.rem(lax.rem(me, spread) + k, spread)
        top, left = tile(h)
        return pltpu.make_async_remote_copy(
            src_ref=t_v.at[a, :, top, left],
            dst_ref=first[a].at[slot_of(me)],
            send_sem=send1.at[a, k],
            recv_sem=recv1.at[a, k],
            device_id={"seq": h},
        )

    def own1(a):
        top, left = tile(me)
        return pltpu.make_async_copy(
            t_v.at[a, :, top, left], first[a].at[slot_of(me)], own_sem.at[a]
        )

    def hand2(a, k):
        d = lax.rem(me + k, n)
        top, left = tile(me)
        return pltpu.make_async_remote_copy(
            src_ref=second.at[a, pl.ds(d * most_pages, most_pages)],
            dst_ref=landing[a].at[pl.ds(my_block * most_pages, most_pages), top, left],
            send_sem=send2.at[a, k],
            recv_sem=recv2.at[a, k],
            device_id={"seq": d},
        )

    def own2(a):
        top, left = tile(me)
        return pltpu.make_async_copy(
            second.at[a, pl.ds(me * most_pages, most_pages)],
            landing[a].at[pl.ds(my_block * most_pages, most_pages), top, left],
            own_sem.at[2 + a],
        )

    loads[0].wait()
    loads[1].wait()
    pl.semaphore_wait(barrier, n - 1)
    for a in range(2):

        @pl.loop(1, spread)
        def _(k, a=a):
            hand1(a, k).start()

        own1(a).start()

    loads[2].wait()
    for s in range(steps):
        qf[pl.ds(s * slots_here, slots_here), :] = q_v[s].astype(F32)

    tokens = pages_here * page_rows
    col = lax.broadcasted_iota(jnp.int32, (1, tokens), 1)
    col_page = col // page_rows
    col_row = col % page_rows
    lines = []
    for r in range(slots_here):
        room = jnp.zeros((1, tokens), jnp.int32)
        for c in range(cache_pages):
            left_over = cached_ref[r] - c * page_rows
            room = jnp.where(col_page == table_ref[r, c], left_over, room)
        lines.append(jnp.where(col_row < room, 0.0, NEG).astype(F32))
    bias = jnp.concatenate(lines * (rows_sr // slots_here), axis=0)
    factor = math.log2(math.e) / math.sqrt(HD)

    def group_queries(g):
        parts = [qf[:, pl.ds((g * share + e) * HD, HD)] for e in range(share)]
        return jnp.concatenate(parts, axis=0).astype(BF16)

    def scores_of(g, keys, biases):
        raw = lax.dot_general(
            group_queries(g), keys, (((1,), (1,)), ((), ())), preferred_element_type=F32
        )
        shaped = raw.reshape(share, rows_sr, keys.shape[0]) * factor + biases[None]
        return shaped.reshape(share * rows_sr, keys.shape[0])

    def resident(g):
        keys = pk_v[:, :, pl.ds(g * HD, HD)].reshape(tokens, HD)
        values = pv_v[:, :, pl.ds(g * HD, HD)].reshape(tokens, HD)
        score = scores_of(g, keys, bias)
        largest = jnp.max(score, axis=-1, keepdims=True)
        prob = jnp.exp2(score - largest)
        mx[g] = jnp.broadcast_to(largest, mx.shape[1:])
        sm[g] = jnp.broadcast_to(jnp.sum(prob, axis=-1, keepdims=True), sm.shape[1:])
        acc[g] = jnp.dot(prob.astype(BF16), values, preferred_element_type=F32)

    loads[3].wait()
    loads[4].wait()
    half = KVH // 2
    for g in range(half):
        resident(g)

    for a in range(2):

        @pl.loop(1, spread)
        def _(k, a=a):
            hand1(a, k).wait_recv()

        own1(a).wait()
        for i in range(n * most_pages):
            second[a, i] = first[a][pick_s[i]]

        @pl.loop(1, n)
        def _(k, a=a):
            hand2(a, k).start()

        own2(a).start()

    for g in range(half, KVH):
        resident(g)

    loads[5].wait()
    loads[6].wait()
    for a in range(2):
        fresh[a, most_pages] = jnp.concatenate(
            [n_v[a, s].astype(F32) for s in range(steps)], axis=0
        ).astype(BF16)
    extra = fresh_span + rows_sr
    line = lax.broadcasted_iota(jnp.int32, (rows_sr, extra), 0)
    col = lax.broadcasted_iota(jnp.int32, (rows_sr, extra), 1)
    line_slot, line_step = line % slots_here, line // slots_here
    new_at = jnp.maximum(col - fresh_span, 0)
    fine_fresh = (line_slot == my_slot) & (col < my_length)
    fine_new = (
        (col >= fresh_span)
        & (new_at % slots_here == line_slot)
        & (new_at // slots_here <= line_step)
    )
    bias2 = jnp.where(fine_fresh | fine_new, 0.0, NEG).astype(F32)

    place = lax.broadcasted_iota(jnp.int32, (page_rows, kv_width), 0)
    landed = (lk_ref, lv_ref)
    for a in range(2):

        @pl.loop(1, n)
        def _(k, a=a):
            hand2(a, k).wait_recv()

        own2(a).wait()
        for j in range(most_pages):
            if blocks == 1:
                block = 0
            else:
                begin = jnp.int32(0)
                for t in range(turns):
                    begin = jnp.where(
                        lax.div(slots_ref[t], slots_here) == me, start_s[t], begin
                    )
                block = lax.div(lax.rem(jnp.minimum(begin + j, group_pages * n - 1), n), spread)
            page = landing[a][block * most_pages + j]
            kept = jnp.where(place + j * page_rows < my_length, page.astype(F32), 0.0)
            kept = kept.astype(BF16)
            fresh[a, j] = kept
            landed[a][j] = kept

    for g in range(KVH):
        keys = fresh[0, :, :, pl.ds(g * HD, HD)].reshape(extra, HD)
        values = fresh[1, :, :, pl.ds(g * HD, HD)].reshape(extra, HD)
        score = scores_of(g, keys, bias2)
        before = mx[g]
        largest = jnp.maximum(before, jnp.max(score, axis=-1, keepdims=True))
        prob = jnp.exp2(score - largest[:, :extra])
        shrink = jnp.exp2(before - largest)
        total = sm[g] * shrink + jnp.sum(prob, axis=-1, keepdims=True)
        mixed = acc[g] * shrink + jnp.dot(
            prob.astype(BF16), values, preferred_element_type=F32
        )
        result = mixed / total
        for e in range(share):
            of[:, pl.ds((g * share + e) * HD, HD)] = result[e * rows_sr : (e + 1) * rows_sr]
    for s in range(steps):
        out_ref[s] = of[pl.ds(s * slots_here, slots_here), :].astype(BF16)

    for a in range(2):

        @pl.loop(1, spread)
        def _(k, a=a):
            hand1(a, k).wait_send()

        @pl.loop(1, n)
        def _(k, a=a):
            hand2(a, k).wait_send()


def per_device(
    queries,
    new_keys,
    new_values,
    pool_keys,
    pool_values,
    page_table,
    cached_len,
    turn_keys,
    turn_values,
    turn_lengths,
    turn_slot,
):
    n = lax.axis_size("seq")
    steps, slots_here, query_width = queries.shape
    pages_here, page_rows, kv_width = pool_keys.shape
    group_pages = turn_keys.shape[0]
    most_pages = -(-MOSTT // page_rows)
    spread = (page_rows // SUB) * (kv_width // LANES)
    blocks = n // spread
    rows_sr = steps * slots_here
    rows = rows_sr * (QH // KVH)
    paged = (group_pages, page_rows, kv_width)
    smem = pl.BlockSpec(memory_space=pltpu.SMEM)
    anywhere = pl.BlockSpec(memory_space=pl.ANY)
    vmem = pl.BlockSpec(memory_space=pltpu.VMEM)
    landed = jax.ShapeDtypeStruct((most_pages, page_rows, kv_width), BF16)
    attended, landed_keys, landed_values = pl.pallas_call(
        functools.partial(kernel, n),
        out_shape=(jax.ShapeDtypeStruct(queries.shape, BF16), landed, landed),
        in_specs=[smem] * 4 + [anywhere] * 7,
        out_specs=(vmem, vmem, vmem),
        scratch_shapes=[
            pltpu.VMEM(queries.shape, BF16),
            pltpu.VMEM((2,) + new_keys.shape, BF16),
            pltpu.VMEM(pool_keys.shape, BF16),
            pltpu.VMEM(pool_values.shape, BF16),
            pltpu.VMEM((2,) + paged, BF16),
            pltpu.VMEM((spread * group_pages, SUB, LANES), BF16),
            pltpu.VMEM((spread * group_pages, SUB, LANES), BF16),
            pltpu.VMEM((2, n * most_pages, SUB, LANES), BF16),
            pltpu.VMEM((blocks * most_pages, page_rows, kv_width), BF16),
            pltpu.VMEM((blocks * most_pages, page_rows, kv_width), BF16),
            pltpu.VMEM((2, most_pages + 1, page_rows, kv_width), BF16),
            pltpu.VMEM((rows_sr, query_width), F32),
            pltpu.VMEM((rows_sr, query_width), F32),
            pltpu.VMEM((KVH, rows, HD), F32),
            pltpu.VMEM((KVH, rows, HD), F32),
            pltpu.VMEM((KVH, rows, HD), F32),
            pltpu.SMEM(turn_lengths.shape, jnp.int32),
            pltpu.SMEM((n * most_pages,), jnp.int32),
            pltpu.SemaphoreType.DMA((7,)),
            pltpu.SemaphoreType.DMA((4,)),
            pltpu.SemaphoreType.DMA((2, spread)),
            pltpu.SemaphoreType.DMA((2, spread)),
            pltpu.SemaphoreType.DMA((2, n)),
            pltpu.SemaphoreType.DMA((2, n)),
        ],
        compiler_params=pltpu.CompilerParams(
            collective_id=0, has_side_effects=True, vmem_limit_bytes=60 * 1024 * 1024
        ),
    )(
        page_table,
        cached_len,
        turn_lengths,
        turn_slot,
        queries,
        new_keys,
        new_values,
        pool_keys,
        pool_values,
        turn_keys.reshape(paged),
        turn_values.reshape(paged),
    )
    span = most_pages * page_rows
    return (
        attended,
        landed_keys.reshape(1, span, kv_width),
        landed_values.reshape(1, span, kv_width),
    )


def solution(mesh):
    in_specs = (
        P(None, ("groups", "seq"), None),
        P(None, ("groups", "seq"), None),
        P(None, ("groups", "seq"), None),
        P(("groups", "seq"), None, None),
        P(("groups", "seq"), None, None),
        P(("groups", "seq"), None),
        P(("groups", "seq")),
        P(None, ("groups", "seq"), None, None),
        P(None, ("groups", "seq"), None, None),
        P("groups"),
        P("groups"),
    )
    out_specs = (
        P(None, ("groups", "seq"), None),
        P(("groups", "seq"), None, None),
        P(("groups", "seq"), None, None),
    )
    return jax.shard_map(
        per_device, mesh=mesh, in_specs=in_specs, out_specs=out_specs, check_vma=False
    )
```

```python
import functools
import math

import jax
import jax.numpy as jnp
from jax import lax
from jax.experimental import pallas as pl
from jax.experimental.pallas import tpu as pltpu
from jax.sharding import PartitionSpec as P

QH = 64
KVH = 8
HD = 128
MOSTT = 80
SUB = 8
LANES = 128
NEG = -1e30
F32 = jnp.float32
BF16 = jnp.bfloat16


FACTOR = math.log2(math.e) / math.sqrt(HD)


def scores_of(qb, g, keys, biases):
    share = QH // KVH
    parts = [qb[:, pl.ds((g * share + e) * HD, HD)] for e in range(share)]
    rows = jnp.concatenate(parts, axis=0)
    raw = lax.dot_general(rows, keys, (((1,), (1,)), ((), ())), preferred_element_type=F32)
    shaped = raw.reshape(share, biases.shape[0], keys.shape[0]) * FACTOR + biases[None]
    return shaped.reshape(rows.shape[0], keys.shape[0])


def each(first, last):
    if last - first > 32:
        return pl.loop(first, last)

    def run(body):
        for k in range(first, last):
            body(k)

    return run


def finish(
    qb_hbm,
    acc_hbm,
    mx_hbm,
    sm_hbm,
    fresh_hbm,
    bias2_hbm,
    out_ref,
    lk_hbm,
    lv_hbm,
    qb,
    acc,
    mx,
    sm,
    fresh,
    bias2_ref,
    of,
    load_sem,
    sem,
):
    loads = [
        pltpu.make_async_copy(src, dst, load_sem.at[i])
        for i, (src, dst) in enumerate(
            (
                (fresh_hbm.at[0], fresh.at[0]),
                (fresh_hbm.at[1], fresh.at[1]),
                (qb_hbm, qb),
                (bias2_hbm, bias2_ref),
                (mx_hbm, mx),
                (sm_hbm, sm),
                (acc_hbm, acc),
            )
        )
    ]
    for copy in loads:
        copy.start()
    share = QH // KVH
    most_pages = lk_hbm.shape[0]
    rows_sr = qb.shape[0]
    steps, slots_here, _ = out_ref.shape
    extra = bias2_ref.shape[1]
    copies = [
        pltpu.make_async_copy(fresh.at[a, pl.ds(0, most_pages)], ref, sem.at[a])
        for a, ref in enumerate((lk_hbm, lv_hbm))
    ]
    for load, copy in zip(loads, copies):
        load.wait()
        copy.start()
    for load in loads[2:]:
        load.wait()
    bias2 = bias2_ref[...]
    for g in range(KVH):
        keys = fresh[0, :, :, pl.ds(g * HD, HD)].reshape(extra, HD)
        values = fresh[1, :, :, pl.ds(g * HD, HD)].reshape(extra, HD)
        score = scores_of(qb, g, keys, bias2)
        before = mx[:, g : g + 1]
        largest = jnp.maximum(before, jnp.max(score, axis=-1, keepdims=True))
        prob = jnp.exp2(score - largest)
        shrink = jnp.exp2(before - largest)
        total = sm[:, g : g + 1] * shrink + jnp.sum(prob, axis=-1, keepdims=True)
        mixed = acc[g] * shrink + jnp.dot(
            prob.astype(BF16), values, preferred_element_type=F32
        )
        result = mixed / total
        for e in range(share):
            of[:, pl.ds((g * share + e) * HD, HD)] = result[e * rows_sr : (e + 1) * rows_sr]
    for s in range(steps):
        out_ref[s] = of[pl.ds(s * slots_here, slots_here), :].astype(BF16)
    for copy in copies:
        copy.wait()


def kernel(
    n,
    table_ref,
    cached_ref,
    lengths_ref,
    slots_ref,
    q_hbm,
    nk_hbm,
    nv_hbm,
    pk_hbm,
    pv_hbm,
    tk_hbm,
    tv_hbm,
    qb_hbm,
    acc_hbm,
    mx_hbm,
    sm_hbm,
    fresh_hbm,
    bias2_hbm,
    qb,
    acc,
    mx,
    sm,
    fresh,
    bias2_ref,
    q_v,
    n_v,
    pk_v,
    pv_v,
    t_v,
    first_k,
    first_v,
    second,
    landing_k,
    landing_v,
    qf,
    start_s,
    pick_s,
    load_sem,
    out_sem,
    own_sem,
    send1,
    recv1,
    send2,
    recv2,
):
    me = lax.axis_index("seq")
    steps, slots_here, _ = q_hbm.shape
    group_pages, page_rows, kv_width = tk_hbm.shape
    pages_here = pk_hbm.shape[0]
    turns = lengths_ref.shape[0]
    cache_pages = table_ref.shape[1]
    lane_tiles = kv_width // LANES
    spread = (page_rows // SUB) * lane_tiles
    most_pages = -(-MOSTT // page_rows)
    fresh_span = most_pages * page_rows
    blocks = n // spread
    rows_sr = steps * slots_here
    my_block = me // spread
    first = (first_k, first_v)
    landing = (landing_k, landing_v)

    barrier = pltpu.get_barrier_semaphore()

    @each(1, n)
    def _(k):
        pl.semaphore_signal(barrier, inc=1, device_id={"seq": lax.rem(me + k, n)})

    def load(index, src, dst):
        return pltpu.make_async_copy(src, dst, load_sem.at[index])

    loads = [
        load(0, tk_hbm, t_v.at[0]),
        load(1, tv_hbm, t_v.at[1]),
        load(2, q_hbm, q_v),
        load(3, pk_hbm, pk_v),
        load(4, pv_hbm, pv_v),
        load(5, nk_hbm, n_v.at[0]),
        load(6, nv_hbm, n_v.at[1]),
    ]
    for copy in loads:
        copy.start()

    running = jnp.int32(0)
    my_length = jnp.int32(0)
    my_slot = jnp.int32(0)
    for t in range(turns):
        start_s[t] = running
        length = lengths_ref[t]
        slot = slots_ref[t]
        mine = lax.div(slot, slots_here) == me
        my_length = jnp.where(mine, length, my_length)
        my_slot = jnp.where(mine, lax.rem(slot, slots_here), my_slot)
        running = running + lax.div(length + (page_rows - 1), page_rows)

    @pl.loop(0, n)
    def _(d):
        begin = jnp.int32(0)
        for t in range(turns):
            begin = jnp.where(lax.div(slots_ref[t], slots_here) == d, start_s[t], begin)
        for j in range(most_pages):
            page = jnp.minimum(begin + j, group_pages * n - 1)
            row = lax.rem(lax.rem(page, n), spread) * group_pages + lax.div(page, n)
            pick_s[d * most_pages + j] = row

    def tile(h):
        t = lax.rem(h, spread)
        top = pl.multiple_of(lax.div(t, lane_tiles) * SUB, SUB)
        left = pl.multiple_of(lax.rem(t, lane_tiles) * LANES, LANES)
        return pl.ds(top, SUB), pl.ds(left, LANES)

    def slot_of(src):
        return pl.ds(lax.rem(src, spread) * group_pages, group_pages)

    def hand1(a, k):
        h = my_block * spread + lax.rem(lax.rem(me, spread) + k, spread)
        top, left = tile(h)
        return pltpu.make_async_remote_copy(
            src_ref=t_v.at[a, :, top, left],
            dst_ref=first[a].at[slot_of(me)],
            send_sem=send1.at[a, k],
            recv_sem=recv1.at[a, k],
            device_id={"seq": h},
        )

    def own1(a):
        top, left = tile(me)
        return pltpu.make_async_copy(
            t_v.at[a, :, top, left], first[a].at[slot_of(me)], own_sem.at[a]
        )

    def hand2(a, k):
        d = lax.rem(me + k, n)
        top, left = tile(me)
        return pltpu.make_async_remote_copy(
            src_ref=second.at[a, pl.ds(d * most_pages, most_pages)],
            dst_ref=landing[a].at[pl.ds(my_block * most_pages, most_pages), top, left],
            send_sem=send2.at[a, k],
            recv_sem=recv2.at[a, k],
            device_id={"seq": d},
        )

    def own2(a):
        top, left = tile(me)
        return pltpu.make_async_copy(
            second.at[a, pl.ds(me * most_pages, most_pages)],
            landing[a].at[pl.ds(my_block * most_pages, most_pages), top, left],
            own_sem.at[2 + a],
        )

    loads[0].wait()
    loads[1].wait()
    pl.semaphore_wait(barrier, n - 1)
    for a in range(2):

        @each(1, spread)
        def _(k, a=a):
            hand1(a, k).start()

        own1(a).start()

    loads[2].wait()
    for s in range(steps):
        qf[pl.ds(s * slots_here, slots_here), :] = q_v[s].astype(F32)
    qb[...] = qf[...].astype(BF16)

    tokens = pages_here * page_rows
    col = lax.broadcasted_iota(jnp.int32, (1, tokens), 1)
    col_page = col // page_rows
    col_row = col % page_rows
    lines = []
    for r in range(slots_here):
        room = jnp.zeros((1, tokens), jnp.int32)
        for c in range(cache_pages):
            left_over = cached_ref[r] - c * page_rows
            room = jnp.where(col_page == table_ref[r, c], left_over, room)
        lines.append(jnp.where(col_row < room, 0.0, NEG).astype(F32))
    bias = jnp.concatenate(lines * (rows_sr // slots_here), axis=0)
    def resident(g):
        keys = pk_v[:, :, pl.ds(g * HD, HD)].reshape(tokens, HD)
        values = pv_v[:, :, pl.ds(g * HD, HD)].reshape(tokens, HD)
        score = scores_of(qb, g, keys, bias)
        largest = jnp.max(score, axis=-1, keepdims=True)
        prob = jnp.exp2(score - largest)
        mx[:, g : g + 1] = largest
        sm[:, g : g + 1] = jnp.sum(prob, axis=-1, keepdims=True)
        acc[g] = jnp.dot(prob.astype(BF16), values, preferred_element_type=F32)

    loads[3].wait()
    loads[4].wait()
    half = KVH // 2
    for g in range(half):
        resident(g)

    for a in range(2):

        @each(1, spread)
        def _(k, a=a):
            hand1(a, k).wait_recv()

        own1(a).wait()
        for i in range(n * most_pages):
            second[a, i] = first[a][pick_s[i]]

        @each(1, n)
        def _(k, a=a):
            hand2(a, k).start()

        own2(a).start()

    for g in range(half, KVH):
        resident(g)

    loads[5].wait()
    loads[6].wait()
    for a in range(2):
        fresh[a, most_pages] = jnp.concatenate(
            [n_v[a, s].astype(F32) for s in range(steps)], axis=0
        ).astype(BF16)
    extra = fresh_span + rows_sr
    line = lax.broadcasted_iota(jnp.int32, (rows_sr, extra), 0)
    col = lax.broadcasted_iota(jnp.int32, (rows_sr, extra), 1)
    line_slot, line_step = line % slots_here, line // slots_here
    new_at = jnp.maximum(col - fresh_span, 0)
    fine_fresh = (line_slot == my_slot) & (col < my_length)
    fine_new = (
        (col >= fresh_span)
        & (new_at % slots_here == line_slot)
        & (new_at // slots_here <= line_step)
    )
    bias2_ref[...] = jnp.where(fine_fresh | fine_new, 0.0, NEG).astype(F32)

    stores = [
        pltpu.make_async_copy(src, dst, out_sem.at[i])
        for i, (src, dst) in enumerate(
            (
                (qb, qb_hbm),
                (acc, acc_hbm),
                (mx, mx_hbm),
                (sm, sm_hbm),
                (bias2_ref, bias2_hbm),
                (fresh.at[0], fresh_hbm.at[0]),
                (fresh.at[1], fresh_hbm.at[1]),
            )
        )
    ]
    for copy in stores[:5]:
        copy.start()

    place = lax.broadcasted_iota(jnp.int32, (page_rows, kv_width), 0)
    for a in range(2):

        @each(1, n)
        def _(k, a=a):
            hand2(a, k).wait_recv()

        own2(a).wait()
        for j in range(most_pages):
            if blocks == 1:
                block = 0
            else:
                begin = jnp.int32(0)
                for t in range(turns):
                    begin = jnp.where(
                        lax.div(slots_ref[t], slots_here) == me, start_s[t], begin
                    )
                block = lax.div(lax.rem(jnp.minimum(begin + j, group_pages * n - 1), n), spread)
            page = landing[a][block * most_pages + j]
            kept = jnp.where(place + j * page_rows < my_length, page.astype(F32), 0.0)
            fresh[a, j] = kept.astype(BF16)
        stores[5 + a].start()

    for a in range(2):

        @each(1, spread)
        def _(k, a=a):
            hand1(a, k).wait_send()

        @each(1, n)
        def _(k, a=a):
            hand2(a, k).wait_send()

    for copy in stores:
        copy.wait()


def per_device(
    queries,
    new_keys,
    new_values,
    pool_keys,
    pool_values,
    page_table,
    cached_len,
    turn_keys,
    turn_values,
    turn_lengths,
    turn_slot,
):
    n = lax.axis_size("seq")
    steps, slots_here, query_width = queries.shape
    pages_here, page_rows, kv_width = pool_keys.shape
    group_pages = turn_keys.shape[0]
    most_pages = -(-MOSTT // page_rows)
    spread = (page_rows // SUB) * (kv_width // LANES)
    blocks = n // spread
    rows_sr = steps * slots_here
    rows = rows_sr * (QH // KVH)
    paged = (group_pages, page_rows, kv_width)
    smem = pl.BlockSpec(memory_space=pltpu.SMEM)
    hbm = pl.BlockSpec(memory_space=pltpu.HBM)
    vmem = pl.BlockSpec(memory_space=pltpu.VMEM)
    extra = most_pages * page_rows + rows_sr
    parts = pl.pallas_call(
        functools.partial(kernel, n),
        out_shape=(
            jax.ShapeDtypeStruct((rows_sr, query_width), BF16),
            jax.ShapeDtypeStruct((KVH, rows, HD), F32),
            jax.ShapeDtypeStruct((rows, KVH), F32),
            jax.ShapeDtypeStruct((rows, KVH), F32),
            jax.ShapeDtypeStruct((2, most_pages + 1, page_rows, kv_width), BF16),
            jax.ShapeDtypeStruct((rows_sr, extra), F32),
        ),
        in_specs=[smem] * 4 + [hbm] * 7,
        out_specs=(hbm,) * 6,
        scratch_shapes=[
            pltpu.VMEM((rows_sr, query_width), BF16),
            pltpu.VMEM((KVH, rows, HD), F32),
            pltpu.VMEM((rows, KVH), F32),
            pltpu.VMEM((rows, KVH), F32),
            pltpu.VMEM((2, most_pages + 1, page_rows, kv_width), BF16),
            pltpu.VMEM((rows_sr, extra), F32),
            pltpu.VMEM(queries.shape, BF16),
            pltpu.VMEM((2,) + new_keys.shape, BF16),
            pltpu.VMEM(pool_keys.shape, BF16),
            pltpu.VMEM(pool_values.shape, BF16),
            pltpu.VMEM((2,) + paged, BF16),
            pltpu.VMEM((spread * group_pages, SUB, LANES), BF16),
            pltpu.VMEM((spread * group_pages, SUB, LANES), BF16),
            pltpu.VMEM((2, n * most_pages, SUB, LANES), BF16),
            pltpu.VMEM((blocks * most_pages, page_rows, kv_width), BF16),
            pltpu.VMEM((blocks * most_pages, page_rows, kv_width), BF16),
            pltpu.VMEM((rows_sr, query_width), F32),
            pltpu.SMEM(turn_lengths.shape, jnp.int32),
            pltpu.SMEM((n * most_pages,), jnp.int32),
            pltpu.SemaphoreType.DMA((7,)),
            pltpu.SemaphoreType.DMA((7,)),
            pltpu.SemaphoreType.DMA((4,)),
            pltpu.SemaphoreType.DMA((2, spread)),
            pltpu.SemaphoreType.DMA((2, spread)),
            pltpu.SemaphoreType.DMA((2, n)),
            pltpu.SemaphoreType.DMA((2, n)),
        ],
        compiler_params=pltpu.CompilerParams(
            collective_id=0, has_side_effects=True, vmem_limit_bytes=60 * 1024 * 1024
        ),
    )(
        page_table,
        cached_len,
        turn_lengths,
        turn_slot,
        queries,
        new_keys,
        new_values,
        pool_keys,
        pool_values,
        turn_keys.reshape(paged),
        turn_values.reshape(paged),
    )
    landed = jax.ShapeDtypeStruct((most_pages, page_rows, kv_width), BF16)
    attended, landed_keys, landed_values = pl.pallas_call(
        finish,
        out_shape=(jax.ShapeDtypeStruct(queries.shape, BF16), landed, landed),
        in_specs=[hbm] * 6,
        out_specs=(vmem, hbm, hbm),
        scratch_shapes=[
            pltpu.VMEM((rows_sr, query_width), BF16),
            pltpu.VMEM((KVH, rows, HD), F32),
            pltpu.VMEM((rows, KVH), F32),
            pltpu.VMEM((rows, KVH), F32),
            pltpu.VMEM((2, most_pages + 1, page_rows, kv_width), BF16),
            pltpu.VMEM((rows_sr, extra), F32),
            pltpu.VMEM((rows_sr, query_width), F32),
            pltpu.SemaphoreType.DMA((7,)),
            pltpu.SemaphoreType.DMA((2,)),
        ],
        compiler_params=pltpu.CompilerParams(vmem_limit_bytes=60 * 1024 * 1024),
    )(*parts)
    span = most_pages * page_rows
    return (
        attended,
        landed_keys.reshape(1, span, kv_width),
        landed_values.reshape(1, span, kv_width),
    )


def solution(mesh):
    in_specs = (
        P(None, ("groups", "seq"), None),
        P(None, ("groups", "seq"), None),
        P(None, ("groups", "seq"), None),
        P(("groups", "seq"), None, None),
        P(("groups", "seq"), None, None),
        P(("groups", "seq"), None),
        P(("groups", "seq")),
        P(None, ("groups", "seq"), None, None),
        P(None, ("groups", "seq"), None, None),
        P("groups"),
        P("groups"),
    )
    out_specs = (
        P(None, ("groups", "seq"), None),
        P(("groups", "seq"), None, None),
        P(("groups", "seq"), None, None),
    )
    return jax.shard_map(
        per_device, mesh=mesh, in_specs=in_specs, out_specs=out_specs, check_vma=False
    )
```
